32 devices in a mesh: seq: 8 (over z, y), ch: 4 (over x, core).
Axes of the slice: x: 2, y: 2, z: 4, core: 2. Of those that a mesh axis runs over, the one named last changes fastest.
Arguments:
- signal: float32 [1, 65536, 1024], P(None, 'seq', 'ch'), may hold values from -6 to 6
- spectrum: float32 [2, 256, 256, 1024], P(None, 'seq', None, 'ch'), may hold values from -6 to 6
- channel_mode: int32 [1024], P('ch'), may hold values 0 or 1
- skip_gain: float32 [1024], P('ch'), may hold values from -4 to 4
- out_weight: bfloat16 [1024, 1024], P('ch'), may hold values from -0.1875 to 0.1875
Outputs:
- projected: float32 [1, 65536, 1024], P(None, 'seq', 'ch')
The draws below stay inside these ranges and needn't reach their ends.
Inputs may be any that keep to these rules, and one draw needn't show every extreme that they name: `channel_mode`: 1 marks a channel whose 65536 positions are one sequence, 0 a channel whose positions form a 256 x 256 image.
All inputs are finite; a program needn't handle non-finite values. No bound on the sum of `channel_mode` on one device may be relied on, other than what follows from the above.
Results may differ from the reference program's by a relative error of at most 0.017.
Values may be sent and summed in bfloat16 or wider, within the bound.
A program may use at most 192 MiB of HBM per device.

```python
import jax
import jax.numpy as jnp
from jax import lax

BATCH = 1
WIDTH = 1024
ROWS = 256
COLUMNS = 256
LENGTH = 65536
N_CH = 4


def place_ends(values, key, low, high):
    place = [jax.random.randint(jax.random.fold_in(key, axis), (), 0, length) for axis, length in enumerate(values.shape)]
    main_axis = values.shape.index(max(values.shape))
    neighbour = place[:main_axis] + [(place[main_axis] + 1) % values.shape[main_axis]] + place[main_axis + 1:]
    return values.at[tuple(place)].set(low).at[tuple(neighbour)].set(high)


def levels(rng, extent, shards, smallest, largest):
    def one(position, shards_of):
        steps = jax.random.uniform(jax.random.fold_in(jax.random.fold_in(rng, 6), position), (shards_of,), jnp.float32, smallest / len(shards), largest / len(shards))
        return jnp.repeat(jnp.exp(steps), extent[position] // shards_of).reshape((-1,) + (1,) * (len(extent) - position - 1))

    level = one(*shards[0])
    for cut in shards[1:]:
        level = level * one(*cut)
    return level


def centred(stream_key, dims, width, limit, cuts=(), dtype=jnp.bfloat16):
    drawn = width * jax.random.normal(stream_key, dims, jnp.float32)
    if cuts:
        drawn = drawn * levels(stream_key, dims, cuts, -0.22, 0.18)
    return jnp.clip(drawn, -limit, limit).astype(dtype)


def setup_inputs(seed: int = 0) -> dict:
    splits = jax.random.split(jax.random.key(seed), 6)
    signal = centred(splits[0], (BATCH, LENGTH, WIDTH), 1.0, 6.0, ((1, 8), (2, 4)), jnp.float32)
    spectrum = centred(splits[1], (2, ROWS, COLUMNS, WIDTH), 0.7071, 6.0, ((1, 8), (3, 4)), jnp.float32)
    channel_mode = place_ends((jax.random.randint(splits[2], (WIDTH,), 0, 2) < 1).astype(jnp.int32), jax.random.fold_in(splits[2], 1), 0, 1)
    skip_gain = centred(splits[3], (WIDTH,), 1.0, 4.0, ((0, 4),), jnp.float32)
    out_weight = centred(splits[4], (WIDTH, WIDTH), WIDTH ** -0.5, 0.1875, ((0, 4),))
    return {"signal": signal, "spectrum": spectrum, "channel_mode": channel_mode, "skip_gain": skip_gain, "out_weight": out_weight}


def convolve_block(packed):
    signal_block, spectrum_block, mode_block, gain_block = packed
    series = jnp.transpose(signal_block, (0, 2, 1))
    filters = lax.complex(spectrum_block[0], spectrum_block[1])
    filters = jnp.transpose(filters, (2, 0, 1))
    linear_filter = jnp.transpose(filters, (0, 2, 1)).reshape(filters.shape[0], LENGTH)
    linear = jnp.real(jnp.fft.ifft(jnp.fft.fft(series, axis=-1) * linear_filter[None], axis=-1))
    images = series.reshape(series.shape[0], series.shape[1], ROWS, COLUMNS)
    planar = jnp.real(jnp.fft.ifft2(jnp.fft.fft2(images, axes=(-2, -1)) * filters[None], axes=(-2, -1)))
    planar = planar.reshape(series.shape)
    convolved = jnp.where(mode_block[None, :, None] == 1, linear, planar)
    hidden = convolved + gain_block[None, :, None] * series
    return jnp.transpose(hidden, (0, 2, 1)).astype(jnp.float32)


def reference(signal, spectrum, channel_mode, skip_gain, out_weight):
    block_width = WIDTH // N_CH
    signal_parts = jnp.moveaxis(signal.reshape(BATCH, LENGTH, N_CH, block_width), 2, 0)
    spectrum_parts = jnp.moveaxis(spectrum.reshape(2, ROWS, COLUMNS, N_CH, block_width), 3, 0)
    mode_parts = channel_mode.reshape(N_CH, block_width)
    gain_parts = skip_gain.reshape(N_CH, block_width)
    hidden_parts = lax.map(convolve_block, (signal_parts, spectrum_parts, mode_parts, gain_parts))
    hidden_parts = hidden_parts.astype(jnp.bfloat16)
    weight_parts = out_weight.reshape(N_CH, block_width, WIDTH)

    def add_block(running, packed):
        features, weights = packed
        partial_value = jnp.dot(features.reshape(BATCH * LENGTH, block_width), weights, preferred_element_type=jnp.float32)
        partial_value = lax.optimization_barrier(partial_value.astype(jnp.bfloat16))
        return running + partial_value.astype(jnp.float32), jnp.zeros((), jnp.float32)

    initial = jnp.zeros((BATCH * LENGTH, WIDTH), jnp.float32)
    total, unused = lax.scan(add_block, initial, (hidden_parts, weight_parts))
    return total.reshape(BATCH, LENGTH, WIDTH)
```

```python
import functools

import jax
import jax.numpy as jnp
import numpy as np
from jax import lax
from jax.experimental import pallas as pl
from jax.experimental.pallas import tpu as pltpu
from jax.sharding import PartitionSpec as P

MESH = pl.DeviceIdType.MESH
LANES = 128
AHEAD = 4
BEHIND = 6
LOW = jnp.bfloat16


def phases(row_count, col_count, period):
    product = np.arange(row_count)[:, None] * np.arange(col_count)[None, :] % period
    angles = product * (2.0 * np.pi / period)
    return np.cos(angles), np.sin(angles)


def tables(rows, columns):
    length = rows * columns
    rc, rs = phases(rows, rows, rows)
    cc, cs = phases(columns, columns, columns)
    first = np.concatenate([rc, -rs], 0)
    forward = np.block([[cc, -cs], [cs, cc]])
    backward = np.block([[cc, cs], [-cs, cc]])
    last = np.concatenate([rc, -rs], 1) / length
    twist = phases(rows, columns, length)
    return tuple(jnp.asarray(t, LOW) for t in (first, forward, backward, last)) + tuple(
        jnp.asarray(t, jnp.float32) for t in twist
    )


def dot(a, b):
    return jnp.dot(a, b, preferred_element_type=jnp.float32)


def filter_image(image, real, imag, linear, tables_refs):
    first_ref, forward_ref, backward_ref, last_ref, tc_ref, ts_ref = tables_refs
    rows, columns = tc_ref.shape
    tc = jnp.where(linear, tc_ref[...], 1.0)
    ts = jnp.where(linear, ts_ref[...], 0.0)
    y = dot(first_ref[...], image)
    yr, yi = y[:rows], y[rows:]
    y = jnp.concatenate([(yr * tc + yi * ts).astype(LOW), (yi * tc - yr * ts).astype(LOW)], 1)
    z = dot(y, forward_ref[...])
    zr, zi = z[:, :columns], z[:, columns:]
    fr = real.astype(jnp.float32)
    fi = imag.astype(jnp.float32)
    g = jnp.concatenate([(zr * fr - zi * fi).astype(LOW), (zr * fi + zi * fr).astype(LOW)], 1)
    u = dot(g, backward_ref[...])
    ur, ui = u[:, :columns], u[:, columns:]
    v = jnp.concatenate([(ur * tc - ui * ts).astype(LOW), (ur * ts + ui * tc).astype(LOW)], 0)
    return dot(last_ref[...], v).astype(LOW)


def exchange_kernel(
    n, m, group,
    sig_ref, spec_ref, mode_ref, gain_ref, weight_ref, *rest,
):
    table_hbm = rest[:6]
    hidden_ref, spread_ref = rest[6:8]
    (
        stage, turned, packed, recv, conv, back, lined, hid,
        t0, t1, t2, t3, t4, t5,
        stage_sem, table_sem, send_sem, recv_sem, bsend_sem, brecv_sem,
        gsend_sem, grecv_sem, own_sem, wsend_sem, wrecv_sem, wown_sem,
    ) = rest[8:]
    table_refs = (t0, t1, t2, t3, t4, t5)
    rows_local, columns, owned = sig_ref.shape
    chunk = n * group
    chunks = owned // chunk
    blocks = owned // LANES
    per_block = LANES // chunk
    halves = columns // LANES
    pitch = turned.shape[0] // (halves * rows_local)
    line_pitch = lined.shape[0] // (halves * chunk)
    cols = spread_ref.shape[3]
    me = lax.axis_index("seq")
    mine = lax.axis_index("ch")

    def load(step):
        b, p = divmod(step, 3)
        lanes = pl.ds(b * LANES, LANES)
        src = sig_ref.at[:, :, lanes] if p == 0 else spec_ref.at[p - 1, :, :, lanes]
        return pltpu.make_async_copy(src, stage.at[step % 2], stage_sem.at[step % 2])

    load(0).start()
    load(1).start()
    for k, ref in enumerate(table_refs):
        pltpu.make_async_copy(table_hbm[k], ref, table_sem.at[k]).start()

    barrier = pltpu.get_barrier_semaphore()
    for k in range(1, n):
        pl.semaphore_signal(barrier, 1, device_id=(lax.rem(me + k, n), mine), device_id_type=MESH)
    for k in range(1, m):
        pl.semaphore_signal(barrier, 1, device_id=(me, lax.rem(mine + k, m)), device_id_type=MESH)
    pl.semaphore_wait(barrier, n + m - 2)

    def weight_cols(g):
        return weight_ref.at[:, :, pl.ds(pl.multiple_of(g * cols, LANES), cols)]

    own_weight = pltpu.make_async_copy(weight_cols(mine), spread_ref.at[:, mine], wown_sem)

    def send_weights():
        own_weight.start()
        for k in range(1, m):
            g = lax.rem(mine + k, m)
            pltpu.make_async_remote_copy(
                weight_cols(g), spread_ref.at[:, mine], wsend_sem, wrecv_sem,
                device_id=(me, g), device_id_type=MESH,
            ).start()

    def pack(step):
        b, p = divmod(step, 3)
        load(step).wait()
        slot = step % 2

        def turn(a, carry):
            t = stage[slot, a].T
            for h in range(halves):
                at = pl.multiple_of((h * rows_local + a) * pitch, 8)
                turned[pl.ds(at, LANES), :] = t[:, h * LANES : (h + 1) * LANES]
            return carry

        lax.fori_loop(0, rows_local, turn, 0)

        def split(jj, carry):
            j = b * per_block + jj
            for q in range(chunk):
                for h in range(halves):
                    v = turned[pl.ds(h * rows_local * pitch + jj * chunk + q, rows_local, stride=pitch), :]
                    packed[p, j, q // group, q % group, :, h * LANES : (h + 1) * LANES] = v.astype(LOW)
            recv[p, j, me] = packed[p, j, me]
            return carry

        lax.fori_loop(0, per_block, split, 0)
        if step + 2 < 3 * blocks:
            load(step + 2).start()

    def send(j, planes):
        for k in range(1, n):
            d = lax.rem(me + k, n)
            pltpu.make_async_remote_copy(
                packed.at[planes, j, d], recv.at[planes, j, me], send_sem, recv_sem.at[j],
                device_id=(d, mine), device_id_type=MESH,
            ).start()

    def convolve(j):
        for i in range(group):
            linear = mode_ref[j * chunk + me * group + i] == 1
            planes = [recv[p, j, :, i].reshape(n * rows_local, columns) for p in range(3)]
            out = filter_image(*planes, linear, table_refs)
            conv[j, :, i] = out.reshape(n, rows_local, columns)
        back[j, me] = conv[j, me]
        for k in range(1, n):
            d = lax.rem(me + k, n)
            pltpu.make_async_remote_copy(
                conv.at[j, d], back.at[j, me], bsend_sem, brecv_sem.at[j],
                device_id=(d, mine), device_id_type=MESH,
            ).start()

    def finish(j):
        for q in range(chunk):
            v = back[j, q // group, q % group].astype(jnp.float32)
            x = packed[0, j, q // group, q % group].astype(jnp.float32)
            v = v + gain_ref[j * chunk + q] * x
            for h in range(halves):
                lined[pl.ds((h * chunk + q) * line_pitch, rows_local), :] = v[:, h * LANES : (h + 1) * LANES]
        for a in range(rows_local):
            for h in range(halves):
                v = lined[pl.ds(h * chunk * line_pitch + a, chunk, stride=line_pitch), :]
                hid[j, :, pl.ds(a * columns + h * LANES, LANES)] = v.astype(LOW)
        pltpu.make_async_copy(hid.at[j], hidden_ref.at[j, mine], own_sem).start()
        for k in range(1, m):
            g = lax.rem(mine + k, m)
            pltpu.make_async_remote_copy(
                hid.at[j], hidden_ref.at[j, mine], gsend_sem, grecv_sem,
                device_id=(me, g), device_id_type=MESH,
            ).start()

    def await_bytes(ref, sem):
        pltpu.make_async_copy(ref, ref, sem).wait()

    pack(0)
    for j in range(per_block):
        send(j, pl.ds(0, 1))
    send_weights()
    pack(1)
    pack(2)
    for j in range(AHEAD):
        send(j, pl.ds(1, 2))
    for step in range(3, 3 * blocks):
        pack(step)
    for k, ref in enumerate(table_refs):
        pltpu.make_async_copy(table_hbm[k], ref, table_sem.at[k]).wait()

    def take(j):
        await_bytes(recv.at[:, j, pl.ds(0, n - 1)], recv_sem.at[j])
        convolve(j)

    def put(j):
        await_bytes(back.at[j, pl.ds(0, n - 1)], brecv_sem.at[j])
        finish(j)

    def step(j, carry):
        take(j)

        @pl.when(j + AHEAD < per_block)
        def _():
            send(j + AHEAD, pl.ds(1, 2))

        @pl.when((j + AHEAD >= per_block) & (j + AHEAD < chunks))
        def _():
            send(j + AHEAD, pl.ds(0, 3))

        @pl.when(j >= BEHIND)
        def _():
            put(j - BEHIND)

        return carry

    lax.fori_loop(0, chunks, step, 0)

    def drain(j, carry):
        put(j)
        return carry

    lax.fori_loop(chunks - BEHIND, chunks, drain, 0)
    own_weight.wait()
    await_bytes(hidden_ref.at[:, 0], own_sem)
    await_bytes(packed.at[:, :, pl.ds(0, n - 1)], send_sem)
    await_bytes(conv.at[:, pl.ds(0, n - 1)], bsend_sem)
    await_bytes(spread_ref.at[:, pl.ds(0, m - 1)], wsend_sem)
    await_bytes(spread_ref.at[:, pl.ds(0, m - 1)], wrecv_sem)
    await_bytes(hidden_ref.at[:, pl.ds(0, m - 1)], gsend_sem)
    await_bytes(hidden_ref.at[:, pl.ds(0, m - 1)], grecv_sem)


def exchange(n, m, signal, spectrum, modes, gains, weights, consts):
    rows_local, columns, owned = signal.shape
    rows = rows_local * n
    group = max(1, 16 // n)
    chunk = n * group
    chunks = owned // chunk
    halves = columns // LANES
    cols = weights.shape[2] // m
    pitch = LANES + 8
    line_pitch = rows_local + 8
    hbm = pl.BlockSpec(memory_space=pl.ANY)
    smem = pl.BlockSpec(memory_space=pltpu.SMEM)
    dma = pltpu.SemaphoreType.DMA
    images = (n, group, rows_local, columns)
    return pl.pallas_call(
        functools.partial(exchange_kernel, n, m, group),
        out_shape=(
            jax.ShapeDtypeStruct((chunks, m, chunk, rows_local * columns), LOW),
            jax.ShapeDtypeStruct((chunks, m, chunk, cols), LOW),
        ),
        in_specs=[hbm, hbm, smem, smem, hbm] + [hbm] * 6,
        out_specs=(hbm, hbm),
        scratch_shapes=[
            pltpu.VMEM((2, rows_local, columns, LANES), jnp.float32),
            pltpu.VMEM((halves * rows_local * pitch, LANES), jnp.float32),
            pltpu.VMEM((3, chunks) + images, LOW),
            pltpu.VMEM((3, chunks) + images, LOW),
            pltpu.VMEM((chunks,) + images, LOW),
            pltpu.VMEM((chunks,) + images, LOW),
            pltpu.VMEM((halves * chunk * line_pitch, LANES), jnp.float32),
            pltpu.VMEM((chunks, chunk, rows_local * columns), LOW),
        ]
        + [pltpu.VMEM(t.shape, t.dtype) for t in consts]
        + [
            dma((2,)), dma((6,)), dma(()), dma((chunks,)), dma(()), dma((chunks,)),
            dma(()), dma(()), dma(()), dma(()), dma(()), dma(()),
        ],
        compiler_params=pltpu.CompilerParams(
            collective_id=0, has_side_effects=True, vmem_limit_bytes=62 * 1024 * 1024
        ),
        cost_estimate=pl.CostEstimate(
            flops=owned // n * 24 * rows * rows * columns,
            bytes_accessed=16 * owned * rows_local * columns,
            transcendentals=0,
        ),
        name="exchange",
    )(signal, spectrum, modes, gains, weights, *consts)


def project_kernel(hidden_ref, weight_ref, out_ref):
    depth = weight_ref.shape[0]
    hidden = hidden_ref[...].reshape(depth, out_ref.shape[0])
    out_ref[...] = lax.dot_general(
        hidden, weight_ref[...], (((0,), (0,)), ((), ())), preferred_element_type=jnp.float32
    )


def project(hidden, weights):
    chunks, m, chunk, positions = hidden.shape
    cols = weights.shape[-1]
    tile = 512
    depth = chunks * m * chunk
    return pl.pallas_call(
        project_kernel,
        grid=(positions // tile,),
        in_specs=[
            pl.BlockSpec((chunks, m, chunk, tile), lambda t: (0, 0, 0, t)),
            pl.BlockSpec((depth, cols), lambda t: (0, 0)),
        ],
        out_specs=pl.BlockSpec((tile, cols), lambda t: (t, 0)),
        out_shape=jax.ShapeDtypeStruct((positions, cols), jnp.float32),
        compiler_params=pltpu.CompilerParams(vmem_limit_bytes=32 * 1024 * 1024),
        name="project",
    )(hidden, weights.reshape(depth, cols))


def per_device(signal, spectrum, channel_mode, skip_gain, out_weight):
    n = lax.axis_size("seq")
    m = lax.axis_size("ch")
    batches, local_len, owned = signal.shape
    rows_local, columns = spectrum.shape[1], spectrum.shape[2]
    chunk = n * max(1, 16 // n)
    consts = tables(rows_local * n, columns)
    weights = out_weight.reshape(owned // chunk, chunk, out_weight.shape[1])
    hidden, spread = exchange(
        n, m, signal.reshape(rows_local, columns, owned), spectrum, channel_mode, skip_gain, weights, consts
    )
    out = project(hidden, spread)
    return out.reshape(batches, local_len, out.shape[1])


def solution(mesh):
    placed = (P(None, "seq", "ch"), P(None, "seq", None, "ch"), P("ch"), P("ch"), P("ch", None))
    return jax.shard_map(
        per_device, mesh=mesh, in_specs=placed, out_specs=P(None, "seq", "ch"), check_vma=False
    )
```

```python
import functools

import jax
import jax.numpy as jnp
import numpy as np
from jax import lax
from jax.experimental import pallas as pl
from jax.experimental.pallas import tpu as pltpu
from jax.sharding import PartitionSpec as P

MESH = pl.DeviceIdType.MESH
LANES = 128
AHEAD = 2
BEHIND = 2
LOW = jnp.bfloat16


def phases(row_count, col_count, period):
    product = np.arange(row_count)[:, None] * np.arange(col_count)[None, :] % period
    angles = product * (2.0 * np.pi / period)
    return np.cos(angles), np.sin(angles)


def tables(rows, columns):
    length = rows * columns
    rc, rs = phases(rows, rows, rows)
    cc, cs = phases(columns, columns, columns)
    first = np.concatenate([rc, -rs], 0)
    forward = np.block([[cc, -cs], [cs, cc]])
    backward = np.block([[cc, cs], [-cs, cc]])
    last = np.concatenate([rc, -rs], 1) / length
    twist = phases(rows, columns, length)
    return tuple(jnp.asarray(t, LOW) for t in (first, forward, backward, last)) + tuple(
        jnp.asarray(t, jnp.float32) for t in twist
    )


def dot(a, b):
    return jnp.dot(a, b, preferred_element_type=jnp.float32)


def filter_image(image, real, imag, linear, tables_refs):
    first_ref, forward_ref, backward_ref, last_ref, tc_ref, ts_ref = tables_refs
    rows, columns = tc_ref.shape
    tc = jnp.where(linear, tc_ref[...], 1.0)
    ts = jnp.where(linear, ts_ref[...], 0.0)
    y = dot(first_ref[...], image)
    yr, yi = y[:rows], y[rows:]
    y = jnp.concatenate([(yr * tc + yi * ts).astype(LOW), (yi * tc - yr * ts).astype(LOW)], 1)
    z = dot(y, forward_ref[...])
    zr, zi = z[:, :columns], z[:, columns:]
    fr = real.astype(jnp.float32)
    fi = imag.astype(jnp.float32)
    g = jnp.concatenate([(zr * fr - zi * fi).astype(LOW), (zr * fi + zi * fr).astype(LOW)], 1)
    u = dot(g, backward_ref[...])
    ur, ui = u[:, :columns], u[:, columns:]
    v = jnp.concatenate([(ur * tc - ui * ts).astype(LOW), (ur * ts + ui * tc).astype(LOW)], 0)
    return dot(last_ref[...], v).astype(LOW)


def exchange_kernel(
    n, m, group,
    sig_ref, spec_ref, mode_ref, gain_ref, weight_ref, *rest,
):
    table_hbm = rest[:6]
    total_ref, late_ref, late_weight_ref = rest[6:9]
    (
        stage, turned, packed, recv, back, lined, spread, weights,
        t0, t1, t2, t3, t4, t5,
        stage_sem, table_sem, send_sem, recv_sem, bsend_sem, brecv_sem,
        gsend_sem, cross_sem, pair_sem, wsend_sem, wrecv_sem, wown_sem, out_sem,
    ) = rest[9:]
    table_refs = (t0, t1, t2, t3, t4, t5)
    rows_local, columns, owned = sig_ref.shape
    chunk = n * group
    chunks = owned // chunk
    blocks = owned // LANES
    per_block = LANES // chunk
    halves = columns // LANES
    pitch = turned.shape[0] // (halves * rows_local)
    line_pitch = lined.shape[0] // (halves * chunk)
    cols = weights.shape[3]
    col_halves = cols // LANES
    depth = m * chunk
    me = lax.axis_index("seq")
    mine = lax.axis_index("ch")
    pair = mine + 1 - 2 * lax.rem(mine, 2)
    across = [lax.rem(mine + 2 * k, m) for k in range(1, m // 2)]
    conv = recv.at[0]

    def load(step):
        b, p = divmod(step, 3)
        lanes = pl.ds(b * LANES, LANES)
        src = sig_ref.at[:, :, lanes] if p == 0 else spec_ref.at[p - 1, :, :, lanes]
        return pltpu.make_async_copy(src, stage.at[step % 2], stage_sem.at[step % 2])

    load(0).start()
    load(1).start()
    barrier = pltpu.get_barrier_semaphore()
    for k in range(1, n):
        pl.semaphore_signal(barrier, 1, device_id=(lax.rem(me + k, n), mine), device_id_type=MESH)
    for k in range(1, m):
        pl.semaphore_signal(barrier, 1, device_id=(me, lax.rem(mine + k, m)), device_id_type=MESH)
    for k, ref in enumerate(table_refs):
        pltpu.make_async_copy(table_hbm[k], ref, table_sem.at[k]).start()

    def weight_cols(g):
        return weight_ref.at[:, :, pl.ds(pl.multiple_of(g * cols, LANES), cols)]

    own_weight = pltpu.make_async_copy(weight_cols(mine), weights.at[:, mine], wown_sem)

    def send_weights():
        own_weight.start()
        for k in range(1, m):
            g = lax.rem(mine + k, m)
            pltpu.make_async_remote_copy(
                weight_cols(g), weights.at[:, mine], wsend_sem, wrecv_sem,
                device_id=(me, g), device_id_type=MESH,
            ).start()

    def turn_all(slot):
        def turn(a, carry):
            t = stage[slot, a].T
            for h in range(halves):
                at = pl.multiple_of((h * rows_local + a) * pitch, 8)
                turned[pl.ds(at, LANES), :] = t[:, h * LANES : (h + 1) * LANES]
            return carry

        lax.fori_loop(0, rows_local, turn, 0)

    def split_all(b, p, after):
        def split(jj, carry):
            j = b * per_block + jj
            for q in range(chunk):
                for h in range(halves):
                    v = turned[pl.ds(h * rows_local * pitch + jj * chunk + q, rows_local, stride=pitch), :]
                    packed[p, j, q // group, q % group, :, h * LANES : (h + 1) * LANES] = v.astype(LOW)
            recv[p, j, me] = packed[p, j, me]
            if after is not None:
                after(j)
            return carry

        lax.fori_loop(0, per_block, split, 0)

    def pack(step, before=None, after=None):
        b, p = divmod(step, 3)
        load(step).wait()
        turn_all(step % 2)
        if before is not None:
            before()
        if step + 2 < 3 * blocks:
            load(step + 2).start()
        split_all(b, p, after)

    def send(j, planes):
        for k in range(1, n):
            d = lax.rem(me + k, n)
            pltpu.make_async_remote_copy(
                packed.at[planes, j, d], recv.at[planes, j, me], send_sem, recv_sem.at[j],
                device_id=(d, mine), device_id_type=MESH,
            ).start()

    def convolve(j):
        for i in range(group):
            linear = mode_ref[j * chunk + me * group + i] == 1
            planes = [recv[p, j, :, i].reshape(n * rows_local, columns) for p in range(3)]
            out = filter_image(*planes, linear, table_refs)
            conv[j, :, i] = out.reshape(n, rows_local, columns)
        back[j, me] = conv[j, me]
        for k in range(1, n):
            d = lax.rem(me + k, n)
            pltpu.make_async_remote_copy(
                conv.at[j, d], back.at[j, me], bsend_sem, brecv_sem.at[j],
                device_id=(d, mine), device_id_type=MESH,
            ).start()

    def give(j, g, to, sem):
        pltpu.make_async_remote_copy(
            spread.at[j, g], spread.at[j, g], gsend_sem, sem, device_id=(me, to), device_id_type=MESH
        ).start()

    def finish(j):
        for q in range(chunk):
            v = back[j, q // group, q % group].astype(jnp.float32)
            x = packed[0, j, q // group, q % group].astype(jnp.float32)
            v = v + gain_ref[j * chunk + q] * x
            for h in range(halves):
                lined[pl.ds((h * chunk + q) * line_pitch, rows_local), :] = v[:, h * LANES : (h + 1) * LANES]
        for a in range(rows_local):
            for h in range(halves):
                v = lined[pl.ds(h * chunk * line_pitch + a, chunk, stride=line_pitch), :]
                spread[j, mine, :, pl.ds(a * columns + h * LANES, LANES)] = v.astype(LOW)
        for g in across:
            give(j, mine, g, cross_sem.at[j])
        give(j, mine, pair, pair_sem.at[j])

    def await_bytes(ref, sem):
        pltpu.make_async_copy(ref, ref, sem).wait()

    def take(j):
        await_bytes(recv.at[:, j, pl.ds(0, n - 1)], recv_sem.at[j])
        convolve(j)

    def put(j):
        await_bytes(back.at[j, pl.ds(0, n - 1)], brecv_sem.at[j])
        finish(j)

    def forward(j):
        if across:
            await_bytes(spread.at[j, pl.ds(0, len(across))], cross_sem.at[j])
        for g in across:
            give(j, g, pair, pair_sem.at[j])

    def gathered(j):
        await_bytes(spread.at[j, pl.ds(0, m // 2)], pair_sem.at[j])

    def accumulate(j):
        gathered(j)
        w = weights[j].reshape(depth, cols)

        def tile(a, carry):
            at = pl.multiple_of(a * columns, LANES)
            v = spread[j, :, :, pl.ds(at, columns)].reshape(depth, columns)
            v = lax.dot_general(v, w, (((0,), (0,)), ((), ())), preferred_element_type=jnp.float32)
            for h in range(col_halves):
                stage[h, a] += v[:, h * LANES : (h + 1) * LANES]
            return carry

        lax.fori_loop(0, rows_local, tile, 0)

    pack(0, before=lambda: pl.semaphore_wait(barrier, n + m - 2), after=lambda j: send(j, pl.ds(0, 1)))
    send_weights()
    pack(1)
    pack(2)
    for j in range(AHEAD):
        send(j, pl.ds(1, 2))
    for step in range(3, 3 * blocks):
        pack(step)
    for k, ref in enumerate(table_refs):
        pltpu.make_async_copy(table_hbm[k], ref, table_sem.at[k]).wait()
    own_weight.wait()
    await_bytes(weights.at[:, pl.ds(0, m - 1)], wrecv_sem)
    for h in range(col_halves):
        stage[h] = jnp.zeros(stage.shape[1:], stage.dtype)

    def step(j, carry):
        take(j)

        @pl.when(j + AHEAD < per_block)
        def _():
            send(j + AHEAD, pl.ds(1, 2))

        @pl.when((j + AHEAD >= per_block) & (j + AHEAD < chunks))
        def _():
            send(j + AHEAD, pl.ds(0, 3))

        @pl.when(j >= BEHIND)
        def _():
            put(j - BEHIND)

        @pl.when(j >= BEHIND + 1)
        def _():
            forward(j - BEHIND - 1)

        @pl.when(j >= BEHIND + 2)
        def _():
            accumulate(j - BEHIND - 2)

        return carry

    lax.fori_loop(0, chunks, step, 0)

    def drain(j, carry):
        put(j)

        @pl.when(j >= 1)
        def _():
            forward(j - 1)

        @pl.when(j >= 2)
        def _():
            accumulate(j - 2)

        return carry

    lax.fori_loop(chunks - BEHIND, chunks, drain, 0)
    last = chunks - 1
    accumulate(last - 1)
    outs = [
        pltpu.make_async_copy(stage.at[h], total_ref.at[:, :, pl.ds(h * LANES, LANES)], out_sem)
        for h in range(col_halves)
    ]
    outs.append(pltpu.make_async_copy(weights.at[last], late_weight_ref, out_sem))
    for copy in outs:
        copy.start()
    forward(last)
    gathered(last)
    outs.append(pltpu.make_async_copy(spread.at[last], late_ref, out_sem))
    outs[-1].start()
    await_bytes(packed.at[:, :, pl.ds(0, n - 1)], send_sem)
    await_bytes(conv.at[:, pl.ds(0, n - 1)], bsend_sem)
    await_bytes(weights.at[:, pl.ds(0, m - 1)], wsend_sem)
    await_bytes(spread.at[:, pl.ds(0, m - 1)], gsend_sem)
    for copy in outs:
        copy.wait()


def exchange(n, m, signal, spectrum, modes, gains, weights, consts):
    rows_local, columns, owned = signal.shape
    rows = rows_local * n
    group = max(1, 16 // n)
    chunk = n * group
    chunks = owned // chunk
    halves = columns // LANES
    cols = weights.shape[2] // m
    pitch = LANES + 8
    line_pitch = rows_local + 8
    hbm = pl.BlockSpec(memory_space=pl.ANY)
    smem = pl.BlockSpec(memory_space=pltpu.SMEM)
    dma = pltpu.SemaphoreType.DMA
    images = (n, group, rows_local, columns)
    return pl.pallas_call(
        functools.partial(exchange_kernel, n, m, group),
        out_shape=(
            jax.ShapeDtypeStruct((rows_local, columns, cols), jnp.float32),
            jax.ShapeDtypeStruct((m, chunk, rows_local * columns), LOW),
            jax.ShapeDtypeStruct((m, chunk, cols), LOW),
        ),
        in_specs=[hbm, hbm, smem, smem, hbm] + [hbm] * 6,
        out_specs=(hbm, hbm, hbm),
        scratch_shapes=[
            pltpu.VMEM((2, rows_local, columns, LANES), jnp.float32),
            pltpu.VMEM((halves * rows_local * pitch, LANES), jnp.float32),
            pltpu.VMEM((3, chunks) + images, LOW),
            pltpu.VMEM((3, chunks) + images, LOW),
            pltpu.VMEM((chunks,) + images, LOW),
            pltpu.VMEM((halves * chunk * line_pitch, LANES), jnp.float32),
            pltpu.VMEM((chunks, m, chunk, rows_local * columns), LOW),
            pltpu.VMEM((chunks, m, chunk, cols), LOW),
        ]
        + [pltpu.VMEM(t.shape, t.dtype) for t in consts]
        + [
            dma((2,)), dma((6,)), dma(()), dma((chunks,)), dma(()), dma((chunks,)),
            dma(()), dma((chunks,)), dma((chunks,)), dma(()), dma(()), dma(()), dma(()),
        ],
        compiler_params=pltpu.CompilerParams(
            collective_id=0, has_side_effects=True, vmem_limit_bytes=63 * 1024 * 1024
        ),
        cost_estimate=pl.CostEstimate(
            flops=owned // n * 24 * rows * rows * columns,
            bytes_accessed=16 * owned * rows_local * columns,
            transcendentals=0,
        ),
        name="exchange",
    )(signal, spectrum, modes, gains, weights, *consts)


def project_kernel(total_ref, hidden_ref, weight_ref, out_ref):
    depth = weight_ref.shape[0]
    hidden = hidden_ref[...].reshape(depth, out_ref.shape[0])
    out_ref[...] = total_ref[...] + lax.dot_general(
        hidden, weight_ref[...], (((0,), (0,)), ((), ())), preferred_element_type=jnp.float32
    )


def project(total, hidden, weights):
    m, chunk, positions = hidden.shape
    cols = weights.shape[-1]
    tile = 1024
    depth = m * chunk
    return pl.pallas_call(
        project_kernel,
        grid=(positions // tile,),
        in_specs=[
            pl.BlockSpec((tile, cols), lambda t: (t, 0)),
            pl.BlockSpec((m, chunk, tile), lambda t: (0, 0, t)),
            pl.BlockSpec((depth, cols), lambda t: (0, 0)),
        ],
        out_specs=pl.BlockSpec((tile, cols), lambda t: (t, 0)),
        out_shape=jax.ShapeDtypeStruct((positions, cols), jnp.float32),
        compiler_params=pltpu.CompilerParams(vmem_limit_bytes=63 * 1024 * 1024),
        name="project",
    )(total.reshape(positions, cols), hidden, weights.reshape(depth, cols))


def per_device(signal, spectrum, channel_mode, skip_gain, out_weight):
    n = lax.axis_size("seq")
    m = lax.axis_size("ch")
    batches, local_len, owned = signal.shape
    rows_local, columns = spectrum.shape[1], spectrum.shape[2]
    chunk = n * max(1, 16 // n)
    consts = tables(rows_local * n, columns)
    weights = out_weight.reshape(owned // chunk, chunk, out_weight.shape[1])
    late = exchange(
        n, m, signal.reshape(rows_local, columns, owned), spectrum, channel_mode, skip_gain, weights, consts
    )
    out = project(*late)
    return out.reshape(batches, local_len, out.shape[1])


def solution(mesh):
    placed = (P(None, "seq", "ch"), P(None, "seq", None, "ch"), P("ch"), P("ch"), P("ch", None))
    return jax.shard_map(
        per_device, mesh=mesh, in_specs=placed, out_specs=P(None, "seq", "ch"), check_vma=False
    )
```

```python
import functools

import jax
import jax.numpy as jnp
import numpy as np
from jax import lax
from jax.experimental import pallas as pl
from jax.experimental.pallas import tpu as pltpu
from jax.sharding import PartitionSpec as P

MESH = pl.DeviceIdType.MESH
LANES = 128
AHEAD = 2
BEHIND = 2
SPAN = 16
VMEM_BYTES = 55 * 1024 * 1024
LOW = jnp.bfloat16


def phases(row_count, col_count, period):
    product = np.arange(row_count)[:, None] * np.arange(col_count)[None, :] % period
    angles = product * (2.0 * np.pi / period)
    return np.cos(angles), np.sin(angles)


def tables(rows, columns):
    length = rows * columns
    rc, rs = phases(rows, rows, rows)
    cc, cs = phases(columns, columns, columns)
    first = np.concatenate([rc, -rs], 0)
    forward = np.block([[cc, -cs], [cs, cc]])
    backward = np.block([[cc, cs], [-cs, cc]])
    last = np.concatenate([rc, -rs], 1) / length
    twist = phases(rows, columns, length)
    return tuple(jnp.asarray(t, LOW) for t in (first, forward, backward, last)) + tuple(
        jnp.asarray(t, jnp.float32) for t in twist
    )


def dot(a, b):
    return jnp.dot(a, b, preferred_element_type=jnp.float32)


def filter_image(image, real, imag, linear, tables_refs):
    first_ref, forward_ref, backward_ref, last_ref, tc_ref, ts_ref = tables_refs
    rows, columns = tc_ref.shape
    tc = jnp.where(linear, tc_ref[...], 1.0)
    ts = jnp.where(linear, ts_ref[...], 0.0)
    y = dot(first_ref[...], image)
    yr, yi = y[:rows], y[rows:]
    y = jnp.concatenate([(yr * tc + yi * ts).astype(LOW), (yi * tc - yr * ts).astype(LOW)], 1)
    z = dot(y, forward_ref[...])
    zr, zi = z[:, :columns], z[:, columns:]
    fr = real.astype(jnp.float32)
    fi = imag.astype(jnp.float32)
    g = jnp.concatenate([(zr * fr - zi * fi).astype(LOW), (zr * fi + zi * fr).astype(LOW)], 1)
    u = dot(g, backward_ref[...])
    ur, ui = u[:, :columns], u[:, columns:]
    v = jnp.concatenate([(ur * tc - ui * ts).astype(LOW), (ur * ts + ui * tc).astype(LOW)], 0)
    return dot(last_ref[...], v).astype(LOW)


def exchange_kernel(
    n, m, group,
    sig_ref, spec_ref, mode_ref, gain_ref, weight_ref, *rest,
):
    table_hbm = rest[:6]
    total_ref = rest[6]
    (
        turned, packed, recv, back, lined, spread, weights,
        t0, t1, t2, t3, t4, t5,
        stage_sem, table_sem, send_sem, recv_sem, bsend_sem, brecv_sem,
        gsend_sem, cross_sem, pair_sem, wsend_sem, wrecv_sem, wown_sem,
    ) = rest[7:]
    table_refs = (t0, t1, t2, t3, t4, t5)
    rows_local, columns, owned = sig_ref.shape
    chunk = n * group
    chunks = owned // chunk
    blocks = owned // LANES
    per_block = LANES // chunk
    halves = columns // LANES
    pitch = turned.shape[0] // (halves * rows_local)
    line_pitch = lined.shape[0] // (halves * chunk)
    cols = weights.shape[3]
    depth = m * chunk
    span = min(SPAN, rows_local)
    me = lax.axis_index("seq")
    mine = lax.axis_index("ch")
    pair = mine + 1 - 2 * lax.rem(mine, 2)
    across = [lax.rem(mine + 2 * k, m) for k in range(1, m // 2)]
    conv = recv.at[0]
    stage = [total_ref.at[:, :, pl.ds(h * LANES, LANES)] for h in range(2)]

    def load(step):
        b, p = divmod(step, 3)
        lanes = pl.ds(b * LANES, LANES)
        src = sig_ref.at[:, :, lanes] if p == 0 else spec_ref.at[p - 1, :, :, lanes]
        return pltpu.make_async_copy(src, stage[step % 2], stage_sem.at[step % 2])

    load(0).start()
    load(1).start()
    barrier = pltpu.get_barrier_semaphore()
    for k in range(1, n):
        pl.semaphore_signal(barrier, 1, device_id=(lax.rem(me + k, n), mine), device_id_type=MESH)
    for k in range(1, m):
        pl.semaphore_signal(barrier, 1, device_id=(me, lax.rem(mine + k, m)), device_id_type=MESH)
    for k, ref in enumerate(table_refs):
        pltpu.make_async_copy(table_hbm[k], ref, table_sem.at[k]).start()

    def weight_cols(g):
        return weight_ref.at[:, :, pl.ds(pl.multiple_of(g * cols, LANES), cols)]

    own_weight = pltpu.make_async_copy(weight_cols(mine), weights.at[:, mine], wown_sem)

    def send_weights():
        own_weight.start()
        for k in range(1, m):
            g = lax.rem(mine + k, m)
            pltpu.make_async_remote_copy(
                weight_cols(g), weights.at[:, mine], wsend_sem, wrecv_sem,
                device_id=(me, g), device_id_type=MESH,
            ).start()

    def turn_all(slot):
        def turn(a, carry):
            t = stage[slot][a].T
            for h in range(halves):
                at = pl.multiple_of((h * rows_local + a) * pitch, 8)
                turned[pl.ds(at, LANES), :] = t[:, h * LANES : (h + 1) * LANES]
            return carry

        lax.fori_loop(0, rows_local, turn, 0)

    def split_all(b, p, after):
        def split(jj, carry):
            j = b * per_block + jj
            for q in range(chunk):
                for h in range(halves):
                    v = turned[pl.ds(h * rows_local * pitch + jj * chunk + q, rows_local, stride=pitch), :]
                    packed[p, j, q // group, q % group, :, h * LANES : (h + 1) * LANES] = v.astype(LOW)
            recv[p, j, me] = packed[p, j, me]
            if after is not None:
                after(j)
            return carry

        lax.fori_loop(0, per_block, split, 0)

    def pack(step, before=None, after=None):
        b, p = divmod(step, 3)
        load(step).wait()
        turn_all(step % 2)
        if before is not None:
            before()
        if step + 2 < 3 * blocks:
            load(step + 2).start()
        split_all(b, p, after)

    def send(j, planes):
        for k in range(1, n):
            d = lax.rem(me + k, n)
            pltpu.make_async_remote_copy(
                packed.at[planes, j, d], recv.at[planes, j, me], send_sem, recv_sem.at[j],
                device_id=(d, mine), device_id_type=MESH,
            ).start()

    def convolve(j):
        for i in range(group):
            linear = mode_ref[j * chunk + me * group + i] == 1
            planes = [recv[p, j, :, i].reshape(n * rows_local, columns) for p in range(3)]
            out = filter_image(*planes, linear, table_refs)
            conv[j, :, i] = out.reshape(n, rows_local, columns)
        back[j, me] = conv[j, me]
        for k in range(1, n):
            d = lax.rem(me + k, n)
            pltpu.make_async_remote_copy(
                conv.at[j, d], back.at[j, me], bsend_sem, brecv_sem.at[j],
                device_id=(d, mine), device_id_type=MESH,
            ).start()

    def give(j, g, to, sem):
        pltpu.make_async_remote_copy(
            spread.at[j, g], spread.at[j, g], gsend_sem, sem, device_id=(me, to), device_id_type=MESH
        ).start()

    def finish(j):
        for q in range(chunk):
            v = back[j, q // group, q % group].astype(jnp.float32)
            x = packed[0, j, q // group, q % group].astype(jnp.float32)
            v = v + gain_ref[j * chunk + q] * x
            for h in range(halves):
                lined[pl.ds((h * chunk + q) * line_pitch, rows_local), :] = v[:, h * LANES : (h + 1) * LANES]
        for a in range(rows_local):
            for h in range(halves):
                v = lined[pl.ds(h * chunk * line_pitch + a, chunk, stride=line_pitch), :]
                spread[j, mine, :, pl.ds(a * columns + h * LANES, LANES)] = v.astype(LOW)
        for g in across:
            give(j, mine, g, cross_sem.at[j])
        give(j, mine, pair, pair_sem.at[j])

    def await_bytes(ref, sem):
        pltpu.make_async_copy(ref, ref, sem).wait()

    def take(j):
        await_bytes(recv.at[:, j, pl.ds(0, n - 1)], recv_sem.at[j])
        convolve(j)

    def put(j):
        await_bytes(back.at[j, pl.ds(0, n - 1)], brecv_sem.at[j])
        finish(j)

    def forward(j):
        if across:
            await_bytes(spread.at[j, pl.ds(0, len(across))], cross_sem.at[j])
        for g in across:
            give(j, g, pair, pair_sem.at[j])

    def gathered(j):
        await_bytes(spread.at[j, pl.ds(0, m // 2)], pair_sem.at[j])

    def accumulate(j):
        gathered(j)
        w = weights[j].reshape(depth, cols)

        def tile(a, carry):
            at = pl.multiple_of(a * span * columns, LANES)
            v = spread[j, :, :, pl.ds(at, span * columns)].reshape(depth, span * columns)
            v = lax.dot_general(v, w, (((0,), (0,)), ((), ())), preferred_element_type=jnp.float32)
            total_ref[pl.ds(a * span, span), :, :cols] += v.reshape(span, columns, cols)
            return carry

        lax.fori_loop(0, rows_local // span, tile, 0)

    pack(0, before=lambda: pl.semaphore_wait(barrier, n + m - 2), after=lambda j: send(j, pl.ds(0, 1)))
    send_weights()
    pack(1)
    pack(2)
    for j in range(AHEAD):
        send(j, pl.ds(1, 2))
    for step in range(3, 3 * blocks):
        pack(step)
    for k, ref in enumerate(table_refs):
        pltpu.make_async_copy(table_hbm[k], ref, table_sem.at[k]).wait()
    own_weight.wait()
    await_bytes(weights.at[:, pl.ds(0, m - 1)], wrecv_sem)
    total_ref[...] = jnp.zeros(total_ref.shape, total_ref.dtype)

    def step(j, carry):
        take(j)

        @pl.when(j + AHEAD < per_block)
        def _():
            send(j + AHEAD, pl.ds(1, 2))

        @pl.when((j + AHEAD >= per_block) & (j + AHEAD < chunks))
        def _():
            send(j + AHEAD, pl.ds(0, 3))

        @pl.when(j >= BEHIND)
        def _():
            put(j - BEHIND)

        @pl.when(j >= BEHIND + 1)
        def _():
            forward(j - BEHIND - 1)

        @pl.when(j >= BEHIND + 2)
        def _():
            accumulate(j - BEHIND - 2)

        return carry

    lax.fori_loop(0, chunks, step, 0)

    def drain(j, carry):
        put(j)

        @pl.when(j >= 1)
        def _():
            forward(j - 1)

        @pl.when(j >= 2)
        def _():
            accumulate(j - 2)

        return carry

    lax.fori_loop(chunks - BEHIND, chunks, drain, 0)
    last = chunks - 1
    accumulate(last - 1)
    forward(last)
    accumulate(last)
    await_bytes(packed.at[:, :, pl.ds(0, n - 1)], send_sem)
    await_bytes(conv.at[:, pl.ds(0, n - 1)], bsend_sem)
    await_bytes(weights.at[:, pl.ds(0, m - 1)], wsend_sem)
    await_bytes(spread.at[:, pl.ds(0, m - 1)], gsend_sem)


def exchange(n, m, signal, spectrum, modes, gains, weights, consts):
    rows_local, columns, owned = signal.shape
    rows = rows_local * n
    group = max(1, 16 // n)
    chunk = n * group
    chunks = owned // chunk
    halves = columns // LANES
    cols = weights.shape[2] // m
    pitch = LANES + 8
    line_pitch = rows_local + 8
    hbm = pl.BlockSpec(memory_space=pl.ANY)
    smem = pl.BlockSpec(memory_space=pltpu.SMEM)
    dma = pltpu.SemaphoreType.DMA
    images = (n, group, rows_local, columns)
    return pl.pallas_call(
        functools.partial(exchange_kernel, n, m, group),
        out_shape=pltpu.VMEM((rows_local, columns, max(cols, 2 * LANES)), jnp.float32),
        in_specs=[hbm, hbm, smem, smem, hbm] + [hbm] * 6,
        out_specs=pl.BlockSpec(memory_space=pltpu.VMEM),
        scratch_shapes=[
            pltpu.VMEM((halves * rows_local * pitch, LANES), jnp.float32),
            pltpu.VMEM((3, chunks) + images, LOW),
            pltpu.VMEM((3, chunks) + images, LOW),
            pltpu.VMEM((chunks,) + images, LOW),
            pltpu.VMEM((halves * chunk * line_pitch, LANES), jnp.float32),
            pltpu.VMEM((chunks, m, chunk, rows_local * columns), LOW),
            pltpu.VMEM((chunks, m, chunk, cols), LOW),
        ]
        + [pltpu.VMEM(t.shape, t.dtype) for t in consts]
        + [
            dma((2,)), dma((6,)), dma(()), dma((chunks,)), dma(()), dma((chunks,)),
            dma(()), dma((chunks,)), dma((chunks,)), dma(()), dma(()), dma(()),
        ],
        compiler_params=pltpu.CompilerParams(
            collective_id=0, has_side_effects=True, vmem_limit_bytes=VMEM_BYTES
        ),
        cost_estimate=pl.CostEstimate(
            flops=owned // n * 24 * rows * rows * columns,
            bytes_accessed=16 * owned * rows_local * columns,
            transcendentals=0,
        ),
        name="exchange",
    )(signal, spectrum, modes, gains, weights, *consts)


def per_device(signal, spectrum, channel_mode, skip_gain, out_weight):
    n = lax.axis_size("seq")
    m = lax.axis_size("ch")
    batches, local_len, owned = signal.shape
    rows_local, columns = spectrum.shape[1], spectrum.shape[2]
    chunk = n * max(1, 16 // n)
    consts = tables(rows_local * n, columns)
    weights = out_weight.reshape(owned // chunk, chunk, out_weight.shape[1])
    out = exchange(
        n, m, signal.reshape(rows_local, columns, owned), spectrum, channel_mode, skip_gain, weights, consts
    )
    return out[..., : out_weight.shape[1] // m].reshape(batches, local_len, out_weight.shape[1] // m)


def solution(mesh):
    placed = (P(None, "seq", "ch"), P(None, "seq", None, "ch"), P("ch"), P("ch"), P("ch", None))
    return jax.shard_map(
        per_device, mesh=mesh, in_specs=placed, out_specs=P(None, "seq", "ch"), check_vma=False
    )
```
